32 devices in a mesh: pw: 8 (over z, core), band: 4 (over y, x).
Axes of the slice: x: 2, y: 2, z: 4, core: 2. Of those that a mesh axis runs over, the one named last changes fastest.
Arguments:
- wavefunctions: bfloat16 [2, 4096, 512], P(None, 'pw', 'band'), may hold values from -0.09375 to 0.09375
- miller: int32 [3, 4096], P(None, 'pw'), may hold values from -16 to 16
- reciprocal: float32 [3, 3], replicated, may hold values from -0.15 to 1.15, as said below
- fractional: float32 [3, 32], replicated, may hold values from 0 to 1
- species: int32 [32], replicated, may hold values from 0 to 3
- atom_order: int32 [32], replicated, may hold values from 0 to 31, each once
- radial_widths: float32 [4, 4], replicated, may hold values from 0.003 to 0.02
- onsite_base: float32 [4, 8, 8], replicated, may hold values from -2 to 2
- coupling: float32 [4, 64, 64], replicated, may hold values from -0.75 to 0.75
- occupations: float32 [512], P('band'), may hold values from 0 to 3, as said below
Outputs:
- applied: bfloat16 [2, 4096, 512], P(None, 'pw', 'band')
- onsite_d: float32 [32, 8, 8], P('pw')
The draws below stay inside these ranges and needn't reach their ends.
Inputs may be any that keep to these rules, and one draw needn't show every extreme that they name: `atom_order`: a permutation of the atoms. `reciprocal`: each diagonal entry is 0.85 or more and each other entry 0.15 or less in magnitude. `occupations`: positive.
All inputs are finite; a program needn't handle non-finite values.
Results may differ from the reference program's by a relative error of at most 0.008.
Values may be sent and summed in bfloat16 or wider, within the bound.
A program may use at most 64 MiB of HBM per device.

```python
import math
import jax
import jax.numpy as jnp
from jax import lax

PROJ = 8
SPECIES = 4
NPW = 4096
NBANDS = 512
ATOMS = 32


def draw_occupations(key, part):
    position = jnp.arange(NBANDS, dtype=jnp.float32) / NBANDS
    fermi = 2.0 / (1.0 + jnp.exp((position - 0.8) * 6.0))
    noise = jax.random.uniform(key, (NBANDS,), jnp.float32, 0.8, 1.2)
    return fermi * noise


def draw_reciprocal(key, part):
    offsets = 0.05 * jax.random.truncated_normal(key, -3.0, 3.0, (3, 3), jnp.float32)
    return jnp.eye(3, dtype=jnp.float32) + offsets


def set_ends(drawn, key, least, largest):
    shape = drawn.shape
    index_at = [jax.random.randint(jax.random.fold_in(key, axis), (), 0, shape[axis]) for axis in range(len(shape))]
    drawn = drawn.at[tuple(index_at)].set(least)
    longest = shape.index(max(shape))
    index_at[longest] = (index_at[longest] + 1) % shape[longest]
    return drawn.at[tuple(index_at)].set(largest)


def levels(stream_key, extent, split, low, high):
    loudness, own = 1.0, jax.random.fold_in(stream_key, 6)
    for dim, parts in split:
        steps = jnp.exp(jax.random.uniform(jax.random.fold_in(own, dim), (parts,), jnp.float32, low / len(split), high / len(split)))
        loudness = loudness * jnp.repeat(steps, extent[dim] // parts).reshape([-1 if axis == dim else 1 for axis in range(len(extent))])
    return loudness


def scatter_about(own_key, shape, deviation, bound, pieces=(), kind=jnp.bfloat16):
    factor_of = levels(own_key, shape, pieces, -0.22, 0.18) if pieces else 1.0
    values = jax.random.normal(own_key, shape, jnp.float32) * deviation * factor_of
    return jnp.minimum(jnp.maximum(values, -bound), bound).astype(kind)


def setup_inputs(seed: int = 0) -> dict:
    arg_keys = jax.random.split(jax.random.key(seed), 11)
    wavefunctions = scatter_about(arg_keys[0], (2, NPW, NBANDS), NPW ** -0.5, 0.09375, ((1, 8), (2, 4)))
    miller = set_ends(jax.random.randint(arg_keys[1], (3, NPW), -16, 17), jax.random.fold_in(arg_keys[1], 1), -16, 16).astype(jnp.int32)
    reciprocal = draw_reciprocal(jax.random.fold_in(arg_keys[10], 71), 0)
    fractional = jnp.clip(jax.random.uniform(arg_keys[3], (3, ATOMS), jnp.float32, 0.0, 1.0), 0.0, 1.0)
    species = set_ends(jax.random.randint(arg_keys[4], (ATOMS,), 0, SPECIES), jax.random.fold_in(arg_keys[4], 1), 0, SPECIES - 1).astype(jnp.int32)
    atom_order = jax.random.permutation(arg_keys[5], ATOMS).astype(jnp.int32)
    radial_widths = jnp.clip(jnp.exp(jax.random.uniform(arg_keys[6], (SPECIES, 4), jnp.float32, math.log(0.003), math.log(0.02))), 0.003, 0.02)
    onsite_base = scatter_about(arg_keys[7], (SPECIES, PROJ, PROJ), PROJ ** -0.5, 2.0, (), jnp.float32)
    coupling = scatter_about(arg_keys[8], (SPECIES, PROJ * PROJ, PROJ * PROJ), (PROJ * PROJ) ** -0.5, 0.75, (), jnp.float32)
    occupations = draw_occupations(jax.random.fold_in(arg_keys[10], 71), 0)
    return {"wavefunctions": wavefunctions, "miller": miller, "reciprocal": reciprocal, "fractional": fractional, "species": species, "atom_order": atom_order, "radial_widths": radial_widths, "onsite_base": onsite_base, "coupling": coupling, "occupations": occupations}


HIGH = lax.Precision.HIGHEST


def projector_tile(miller_cols, reciprocal, positions, atom_species, radial_widths):
    two_pi = 2.0 * math.pi
    miller_real = miller_cols.astype(jnp.float32)
    g_vectors = two_pi * jnp.dot(reciprocal, miller_real, precision=HIGH)
    g_square = jnp.sum(g_vectors * g_vectors, axis=0)
    phases = two_pi * jnp.dot(positions.T, miller_real, precision=HIGH)
    onehot = (atom_species[:, None] == jnp.arange(radial_widths.shape[0], dtype=jnp.int32)[None, :]).astype(jnp.float32)
    widths = jnp.dot(onehot, radial_widths, precision=HIGH)
    radial = jnp.exp(-0.5 * g_square[None, None, :] * (widths * widths)[:, :, None])
    s_part = radial[:, 0:2, :]
    p_first = g_vectors[None, :, :] * (widths[:, 2, None, None] * radial[:, 2:3, :])
    p_second = g_vectors[None, :, :] * (widths[:, 3, None, None] * radial[:, 3:4, :])
    p_part = jnp.concatenate([p_first, p_second], axis=1)
    cosine = jnp.cos(phases)[:, None, :]
    sine = jnp.sin(phases)[:, None, :]
    beta_real = jnp.concatenate([s_part * cosine, -p_part * sine], axis=1)
    beta_imag = jnp.concatenate([-s_part * sine, -p_part * cosine], axis=1)
    rows = positions.shape[1] * 8
    return (beta_real.reshape(rows, -1).astype(jnp.bfloat16), beta_imag.reshape(rows, -1).astype(jnp.bfloat16))


def project(beta_real, beta_imag, wave_real, wave_imag):
    proj_real = jnp.dot(beta_real, wave_real, preferred_element_type=jnp.float32) + jnp.dot(beta_imag, wave_imag, preferred_element_type=jnp.float32)
    proj_imag = jnp.dot(beta_real, wave_imag, preferred_element_type=jnp.float32) - jnp.dot(beta_imag, wave_real, preferred_element_type=jnp.float32)
    return jnp.stack([proj_real, proj_imag], axis=1)


def occupancy_terms(projections, weights):
    grouped = projections.reshape(projections.shape[0] // 8, 8, 2, projections.shape[2])
    return jnp.einsum("aicn,ajcn,n->aij", grouped, grouped, weights, precision=HIGH)


def onsite_matrix(occupancy, atom_species, onsite_base, coupling):
    count = occupancy.shape[0]
    kinds = onsite_base.shape[0]
    onehot = (atom_species[:, None] == jnp.arange(kinds, dtype=jnp.int32)[None, :]).astype(jnp.float32)
    response = jnp.einsum("skl,al->ask", coupling, occupancy.reshape(count, 64), precision=HIGH)
    base = jnp.einsum("as,sk->ak", onehot, onsite_base.reshape(kinds, 64), precision=HIGH)
    total = base + jnp.einsum("as,ask->ak", onehot, response, precision=HIGH)
    return total.reshape(count, 8, 8)


def weigh(onsite, projections):
    grouped = projections.reshape(projections.shape[0] // 8, 8, 2, projections.shape[2])
    weighted = jnp.einsum("aij,ajcn->aicn", onsite, grouped, precision=HIGH)
    return weighted.reshape(projections.shape).astype(jnp.bfloat16)


def back_project(beta_real, beta_imag, weighted):
    dims = (((0,), (0,)), ((), ()))
    q_real = weighted[:, 0, :]
    q_imag = weighted[:, 1, :]
    out_real = lax.dot_general(beta_real, q_real, dims, preferred_element_type=jnp.float32) - lax.dot_general(beta_imag, q_imag, dims, preferred_element_type=jnp.float32)
    out_imag = lax.dot_general(beta_real, q_imag, dims, preferred_element_type=jnp.float32) + lax.dot_general(beta_imag, q_real, dims, preferred_element_type=jnp.float32)
    return jnp.stack([out_real, out_imag], axis=0)


def reference(wavefunctions, miller, reciprocal, fractional, species, atom_order, radial_widths, onsite_base, coupling, occupations):
    sorted_species = species[atom_order]
    sorted_positions = fractional[:, atom_order]
    beta_real, beta_imag = projector_tile(miller, reciprocal, sorted_positions, sorted_species, radial_widths)
    projections = project(beta_real, beta_imag, wavefunctions[0], wavefunctions[1])
    weights = occupations / NBANDS
    occupancy = occupancy_terms(projections, weights)
    onsite = onsite_matrix(occupancy, sorted_species, onsite_base, coupling)
    weighted = weigh(onsite, projections)
    applied = back_project(beta_real, beta_imag, weighted).astype(jnp.bfloat16)
    return applied, onsite
```

```python
import functools
import math

import jax
import jax.numpy as jnp
import numpy as np
from jax import lax
from jax.experimental import pallas as pl
from jax.experimental.pallas import tpu as pltpu
from jax.sharding import PartitionSpec as P

MESH = pl.DeviceIdType.MESH
HIGH = lax.Precision.HIGHEST
BF = jnp.bfloat16
F32 = jnp.float32


def even_fit(function, degree):
    nodes = 0.125 + 0.125 * np.cos(np.pi * (np.arange(64) + 0.5) / 64)
    fit = np.polynomial.Chebyshev.fit(nodes, function(np.sqrt(nodes)), degree, domain=[0.0, 0.25])
    return [float(c) for c in fit.convert(kind=np.polynomial.Polynomial, domain=[-1, 1]).coef]


COS = even_fit(lambda t: np.cos(2 * np.pi * t), 7)
SIN = even_fit(lambda t: np.sin(2 * np.pi * t) / t, 7)


def series(coefs, u):
    value = jnp.full_like(u, coefs[-1])
    for c in coefs[-2::-1]:
        value = value * u + c
    return value


def iota(shape, dim):
    return lax.broadcasted_iota(jnp.int32, shape, dim)


def kernel(
    n,
    nb,
    wave,
    miller,
    reciprocal,
    fractional,
    species,
    order,
    widths,
    base,
    coupling,
    occ,
    applied,
    onsite,
    wv,
    xs,
    cs,
    sn,
    amp,
    beta,
    beta_t,
    part,
    rs_in,
    p_all,
    occ_out,
    occ_in,
    d_all,
    ww,
    load_sem,
    rs_s,
    rs_r,
    ag_s,
    ag_r,
    d_s,
    d_r,
    oc_s,
    oc_r,
):
    me = lax.axis_index("pw")
    mb = lax.axis_index("band")
    npw = wave.shape[1]
    bands = wave.shape[2]
    atoms = order.shape[0]
    own = atoms // n
    rows = own * 8
    every = atoms * 8

    barrier = pltpu.get_barrier_semaphore()
    for s in range(1, n):
        pl.semaphore_signal(
            barrier, inc=1, device_id={"pw": lax.rem(me + s, n)}, device_id_type=MESH
        )
    for s in range(1, nb):
        pl.semaphore_signal(
            barrier, inc=1, device_id={"band": lax.rem(mb + s, nb)}, device_id_type=MESH
        )

    loads = [
        pltpu.make_async_copy(wave.at[0], wv.at[pl.ds(0, npw), pl.ds(0, bands)], load_sem.at[0]),
        pltpu.make_async_copy(
            wave.at[1], wv.at[pl.ds(0, npw), pl.ds(bands, bands)], load_sem.at[1]
        ),
        pltpu.make_async_copy(wave.at[1], wv.at[pl.ds(npw, npw), pl.ds(0, bands)], load_sem.at[2]),
    ]
    for copy in loads:
        copy.start()

    m = [miller[c : c + 1, :].astype(F32) for c in range(3)]
    g = [
        (2.0 * math.pi)
        * (reciprocal[c, 0] * m[0] + reciprocal[c, 1] * m[1] + reciprocal[c, 2] * m[2])
        for c in range(3)
    ]
    g2 = g[0] * g[0] + g[1] * g[1] + g[2] * g[2]
    j = iota((8, npw), 0)
    is_s = j < 2
    wide = [jnp.broadcast_to(v, (8, npw)) for v in g]
    factor = jnp.where(
        (j == 2) | (j == 5), wide[0], jnp.where((j == 3) | (j == 6), wide[1], wide[2])
    )
    half = jnp.broadcast_to(-0.5 * g2, (8, npw))
    for s in range(widths.shape[0]):
        w = jnp.where(
            j == 0,
            widths[s, 0],
            jnp.where(j == 1, widths[s, 1], jnp.where(j < 5, widths[s, 2], widths[s, 3])),
        )
        amp[s] = jnp.where(is_s, 1.0, factor * w) * jnp.exp(half * (w * w))

    def position(k, carry):
        a = order[k]
        xs[pl.ds(k, 1), :] = (
            fractional[0, a] * m[0] + fractional[1, a] * m[1] + fractional[2, a] * m[2]
        )
        return carry

    lax.fori_loop(0, atoms, position, 0, unroll=8)
    x = xs[...]
    t = x - jnp.round(x)
    u = t * t
    cs[...] = series(COS, u)
    sn[...] = t * series(SIN, u)

    def projector(pair, carry):
        real, imag = [], []
        for e in range(2):
            k = pair * 2 + e
            c = jnp.broadcast_to(cs[pl.ds(k, 1), :], (8, npw))
            s = jnp.broadcast_to(sn[pl.ds(k, 1), :], (8, npw))
            a = amp[species[order[k]]]
            real.append(a * jnp.where(is_s, c, -s))
            imag.append(-a * jnp.where(is_s, s, c))
        at = pl.ds(pl.multiple_of(pair * 16, 16), 16)
        beta[at, 0:npw] = jnp.concatenate(real, axis=0).astype(BF)
        beta[at, npw : 2 * npw] = jnp.concatenate(imag, axis=0).astype(BF)
        return carry

    lax.fori_loop(0, atoms // 2, projector, 0, unroll=4)

    for copy in loads:
        copy.wait()
    wv[npw : 2 * npw, bands : 2 * bands] = -wv[0:npw, 0:bands]
    part[...] = jnp.dot(beta[...], wv[...], preferred_element_type=F32).astype(BF)
    pl.semaphore_wait(barrier, n - 1 + nb - 1)

    def block(index):
        return pl.ds(pl.multiple_of(index * rows, rows), rows)

    sends = []
    for s in range(1, n):
        to = lax.rem(me + s, n)
        copy = pltpu.make_async_remote_copy(
            src_ref=part.at[block(to)],
            dst_ref=rs_in.at[s],
            send_sem=rs_s.at[s],
            recv_sem=rs_r.at[s],
            device_id={"pw": to},
            device_id_type=MESH,
        )
        copy.start()
        sends.append(copy)

    beta_t[:, 0:every] = beta[:, 0:npw].T
    beta_t[:, every : 2 * every] = beta[:, npw : 2 * npw].T
    weights = occ[...] * (1.0 / (bands * nb))
    weights = jnp.concatenate([weights, weights], axis=1)
    kinds = [species[order[me * own + k]] for k in range(own)]
    base8 = jnp.concatenate([base[kind] for kind in kinds], axis=1)
    spread = (
        (iota((rows, own * 64), 0) // 8 == iota((rows, own * 64), 1) // 64)
        & (iota((rows, own * 64), 0) % 8 == iota((rows, own * 64), 1) % 8)
    ).astype(F32)
    gather = (
        (iota((own * 64, rows), 1) // 8 == iota((own * 64, rows), 0) // 64)
        & (iota((own * 64, rows), 1) % 8 == iota((own * 64, rows), 0) % 8)
    ).astype(F32)
    row_of = (iota((8, own * 64), 1) % 64) // 8 == iota((8, own * 64), 0)
    diagonal = iota((rows, rows), 0) // 8 == iota((rows, rows), 1) // 8

    total = part[block(me), :].astype(F32)
    for s in range(1, n):
        sends[s - 1].wait_recv()
        total = total + rs_in[s].astype(F32)
    p_all[0] = total.astype(BF)
    gram = lax.dot_general(
        total * weights, total, (((1,), (1,)), ((), ())), precision=HIGH, preferred_element_type=F32
    )
    gram = jnp.where(diagonal, gram, 0.0)
    occ8 = gram[0:8, :]
    for k in range(1, own):
        occ8 = occ8 + gram[k * 8 : k * 8 + 8, :]
    occ_out[:, 0:rows] = occ8

    occ_sends = []
    for s in range(1, nb):
        copy = pltpu.make_async_remote_copy(
            src_ref=occ_out,
            dst_ref=occ_in.at[s],
            send_sem=oc_s.at[s],
            recv_sem=oc_r.at[s],
            device_id={"band": lax.rem(mb + s, nb)},
            device_id_type=MESH,
        )
        copy.start()
        occ_sends.append(copy)
    p_sends = []
    for s in range(1, n):
        copy = pltpu.make_async_remote_copy(
            src_ref=p_all.at[0],
            dst_ref=p_all.at[s],
            send_sem=ag_s.at[s],
            recv_sem=ag_r.at[s],
            device_id={"pw": lax.rem(me + s, n)},
            device_id_type=MESH,
        )
        copy.start()
        p_sends.append(copy)

    for copy in occ_sends:
        copy.wait_recv()
    occ_in[0] = occ_out[...]
    occ8 = occ_in[lax.rem(mb + nb, nb)][:, 0:rows]
    for b in range(1, nb):
        occ8 = occ8 + occ_in[lax.rem(mb - b + nb, nb)][:, 0:rows]
    flat = jnp.dot(occ8, spread, precision=HIGH, preferred_element_type=F32)
    flat = jnp.sum(jnp.where(row_of, flat, 0.0), axis=0, keepdims=True)
    answers = []
    for k in range(own):
        line = jnp.broadcast_to(flat[:, k * 64 : k * 64 + 64], (8, 64))
        answers.append(
            lax.dot_general(
                line,
                coupling[kinds[k]],
                (((1,), (1,)), ((), ())),
                precision=HIGH,
                preferred_element_type=F32,
            )
        )
    answer = jnp.where(row_of, jnp.concatenate(answers, axis=1), 0.0)
    d8 = base8 + jnp.dot(answer, gather, precision=HIGH, preferred_element_type=F32)
    d_all[0, :, 0:rows] = d8

    d_sends = []
    for s in range(1, n):
        copy = pltpu.make_async_remote_copy(
            src_ref=d_all.at[0],
            dst_ref=d_all.at[s],
            send_sem=d_s.at[s],
            recv_sem=d_r.at[s],
            device_id={"pw": lax.rem(me + s, n)},
            device_id_type=MESH,
        )
        copy.start()
        d_sends.append(copy)
    for k in range(own):
        onsite[k] = d8[:, k * 8 : k * 8 + 8]

    for s in range(n):
        if s:
            p_sends[s - 1].wait_recv()
            d_sends[s - 1].wait_recv()
        mine = d_all[s][:, 0:rows]
        square = jnp.where(diagonal, jnp.concatenate([mine] * own, axis=0), 0.0)
        upper = square.astype(BF)
        lower = (square - upper.astype(F32)).astype(BF)
        p = p_all[s]
        w = jnp.dot(upper, p, preferred_element_type=F32) + jnp.dot(
            lower, p, preferred_element_type=F32
        )
        w = w.astype(BF)
        owner = lax.rem(me - s + n, n)
        ww[block(owner), :] = w
        second = pl.ds(pl.multiple_of(every + owner * rows, rows), rows)
        ww[second, 0:bands] = -w[:, bands : 2 * bands]
        ww[second, bands : 2 * bands] = w[:, 0:bands]
    result = jnp.dot(beta_t[...], ww[...], preferred_element_type=F32).astype(BF)
    applied[0] = result[:, 0:bands]
    applied[1] = result[:, bands : 2 * bands]
    for copy in sends + occ_sends + p_sends + d_sends:
        copy.wait_send()


def solution(mesh):
    n, nb = mesh.shape["pw"], mesh.shape["band"]

    def local(wave, miller, reciprocal, fractional, species, order, widths, base, coupling, occ):
        _, npw, bands = wave.shape
        atoms = order.shape[0]
        own = atoms // n
        rows, every = own * 8, atoms * 8
        lanes = -(-rows // 128) * 128
        vmem = pl.BlockSpec(memory_space=pltpu.VMEM)
        smem = pl.BlockSpec(memory_space=pltpu.SMEM)
        dma = pltpu.SemaphoreType.DMA
        return pl.pallas_call(
            functools.partial(kernel, n, nb),
            out_shape=(
                jax.ShapeDtypeStruct(wave.shape, BF),
                jax.ShapeDtypeStruct((own, 8, 8), F32),
            ),
            in_specs=[
                pl.BlockSpec(memory_space=pl.ANY),
                vmem,
                smem,
                smem,
                smem,
                smem,
                smem,
                vmem,
                vmem,
                vmem,
            ],
            out_specs=(vmem, vmem),
            scratch_shapes=[
                pltpu.VMEM((2 * npw, 2 * bands), BF),
                pltpu.VMEM((atoms, npw), F32),
                pltpu.VMEM((atoms, npw), F32),
                pltpu.VMEM((atoms, npw), F32),
                pltpu.VMEM((widths.shape[0], 8, npw), F32),
                pltpu.VMEM((every, 2 * npw), BF),
                pltpu.VMEM((npw, 2 * every), BF),
                pltpu.VMEM((every, 2 * bands), BF),
                pltpu.VMEM((n, rows, 2 * bands), BF),
                pltpu.VMEM((n, rows, 2 * bands), BF),
                pltpu.VMEM((8, lanes), F32),
                pltpu.VMEM((nb, 8, lanes), F32),
                pltpu.VMEM((n, 8, lanes), F32),
                pltpu.VMEM((2 * every, 2 * bands), BF),
                dma((3,)),
                dma((n,)),
                dma((n,)),
                dma((n,)),
                dma((n,)),
                dma((n,)),
                dma((n,)),
                dma((nb,)),
                dma((nb,)),
            ],
            compiler_params=pltpu.CompilerParams(collective_id=0, has_side_effects=True),
        )(
            wave,
            miller,
            reciprocal,
            fractional,
            species,
            order,
            widths,
            base,
            coupling,
            occ.reshape(1, bands),
        )

    placed = (P(None, "pw", "band"), P(None, "pw"), P(), P(), P(), P(), P(), P(), P(), P("band"))
    return jax.shard_map(
        local,
        mesh=mesh,
        in_specs=placed,
        out_specs=(P(None, "pw", "band"), P("pw", None, None)),
        check_vma=False,
    )
```

```python
import functools
import math

import jax
import jax.numpy as jnp
import numpy as np
from jax import lax
from jax.experimental import pallas as pl
from jax.experimental.pallas import tpu as pltpu
from jax.sharding import PartitionSpec as P

MESH = pl.DeviceIdType.MESH
HIGH = lax.Precision.HIGHEST
BF = jnp.bfloat16
F32 = jnp.float32


def even_fit(function, degree):
    nodes = 0.125 + 0.125 * np.cos(np.pi * (np.arange(64) + 0.5) / 64)
    fit = np.polynomial.Chebyshev.fit(nodes, function(np.sqrt(nodes)), degree, domain=[0.0, 0.25])
    return [float(c) for c in fit.convert(kind=np.polynomial.Polynomial, domain=[-1, 1]).coef]


COS = even_fit(lambda t: np.cos(2 * np.pi * t), 7)
SIN = even_fit(lambda t: np.sin(2 * np.pi * t) / t, 7)


def series(coefs, u):
    value = jnp.full_like(u, coefs[-1])
    for c in coefs[-2::-1]:
        value = value * u + c
    return value


def iota(shape, dim):
    return lax.broadcasted_iota(jnp.int32, shape, dim)


def kernel(
    n,
    nb,
    wave,
    miller_h,
    reciprocal_h,
    fractional_h,
    species_h,
    order_h,
    widths_h,
    base_h,
    coupling_h,
    occ_h,
    applied,
    onsite,
    miller,
    reciprocal,
    fractional,
    species,
    order,
    widths,
    base,
    coupling,
    occ,
    wv,
    xs,
    cs,
    sn,
    amp,
    beta,
    beta_t,
    part,
    rs_in,
    p_all,
    o_in,
    o_sum,
    respond,
    ww,
    load_sem,
    rs_s,
    rs_r,
    ag_s,
    ag_r,
    oc_s,
    oc_r,
):
    me = lax.axis_index("pw")
    mb = lax.axis_index("band")
    npw = wave.shape[1]
    bands = wave.shape[2]
    atoms = order.shape[0]
    kinds = widths.shape[0]
    own = atoms // n
    pack = own // 2
    rows = own * 8
    every = atoms * 8
    peers = n * nb

    small = [
        (miller_h, miller),
        (reciprocal_h, reciprocal),
        (fractional_h, fractional),
        (species_h, species),
        (order_h, order),
        (widths_h, widths),
        (base_h, base),
        (coupling_h, coupling),
        (occ_h, occ),
        (wave.at[0], wv.at[pl.ds(0, npw), pl.ds(0, bands)]),
        (wave.at[1], wv.at[pl.ds(0, npw), pl.ds(bands, bands)]),
        (wave.at[1], wv.at[pl.ds(npw, npw), pl.ds(0, bands)]),
    ]
    loads = [
        pltpu.make_async_copy(source, to, load_sem.at[i]) for i, (source, to) in enumerate(small)
    ]
    for copy in loads:
        copy.start()
    barrier = pltpu.get_barrier_semaphore()

    def place(q):
        return {"pw": lax.rem(me + q // nb, n), "band": lax.rem(mb + lax.rem(q, nb), nb)}

    def greet(q, carry):
        pl.semaphore_signal(barrier, inc=1, device_id=place(q), device_id_type=MESH)
        return carry

    lax.fori_loop(1, peers, greet, 0)
    for copy in loads[0:6]:
        copy.wait()

    m = [miller[c : c + 1, :].astype(F32) for c in range(3)]
    g = [
        (2.0 * math.pi)
        * (reciprocal[c, 0] * m[0] + reciprocal[c, 1] * m[1] + reciprocal[c, 2] * m[2])
        for c in range(3)
    ]
    g2 = g[0] * g[0] + g[1] * g[1] + g[2] * g[2]
    j = iota((8, npw), 0)
    is_s = j < 2
    wide = [jnp.broadcast_to(v, (8, npw)) for v in g]
    factor = jnp.where(
        (j == 2) | (j == 5), wide[0], jnp.where((j == 3) | (j == 6), wide[1], wide[2])
    )
    half = jnp.broadcast_to(-0.5 * g2, (8, npw))
    for s in range(widths.shape[0]):
        w = jnp.where(
            j == 0,
            widths[s, 0],
            jnp.where(j == 1, widths[s, 1], jnp.where(j < 5, widths[s, 2], widths[s, 3])),
        )
        amp[s] = jnp.where(is_s, 1.0, factor * w) * jnp.exp(half * (w * w))

    def position(k, carry):
        a = order[k]
        xs[pl.ds(k, 1), :] = (
            fractional[0, a] * m[0] + fractional[1, a] * m[1] + fractional[2, a] * m[2]
        )
        return carry

    lax.fori_loop(0, atoms, position, 0, unroll=8)
    x = xs[...]
    t = x - jnp.round(x)
    u = t * t
    cs[...] = series(COS, u)
    sn[...] = t * series(SIN, u)

    def projector(pair, carry):
        real, imag = [], []
        for e in range(2):
            k = pair * 2 + e
            c = jnp.broadcast_to(cs[pl.ds(k, 1), :], (8, npw))
            s = jnp.broadcast_to(sn[pl.ds(k, 1), :], (8, npw))
            a = amp[species[order[k]]]
            real.append(a * jnp.where(is_s, c, -s))
            imag.append(-a * jnp.where(is_s, s, c))
        at = pl.ds(pl.multiple_of(pair * 16, 16), 16)
        beta[at, 0:npw] = jnp.concatenate(real, axis=0).astype(BF)
        beta[at, npw : 2 * npw] = jnp.concatenate(imag, axis=0).astype(BF)
        return carry

    lax.fori_loop(0, atoms // 2, projector, 0, unroll=4)

    for copy in loads[6:]:
        copy.wait()
    wv[npw : 2 * npw, bands : 2 * bands] = -wv[0:npw, 0:bands]
    part[...] = jnp.dot(beta[...], wv[...], preferred_element_type=F32).astype(BF)
    pl.semaphore_wait(barrier, peers - 1)

    def block(index):
        return pl.ds(pl.multiple_of(index * rows, rows), rows)

    sends = []
    for s in range(1, n):
        to = lax.rem(me + s, n)
        copy = pltpu.make_async_remote_copy(
            src_ref=part.at[block(to)],
            dst_ref=rs_in.at[s],
            send_sem=rs_s.at[s],
            recv_sem=rs_r.at[s],
            device_id={"pw": to},
            device_id_type=MESH,
        )
        copy.start()
        sends.append(copy)

    beta_t[:, 0:every] = beta[:, 0:npw].T
    beta_t[:, every : 2 * every] = beta[:, npw : 2 * npw].T
    weights = occ[...] * (1.0 / (bands * nb))
    weights = jnp.concatenate([weights, weights], axis=1)
    spread = (
        (iota((rows, own * 64), 0) // 8 == iota((rows, own * 64), 1) // 64)
        & (iota((rows, own * 64), 0) % 8 == iota((rows, own * 64), 1) % 8)
    ).astype(F32)
    row_of = (iota((8, own * 64), 1) % 64) // 8 == iota((8, own * 64), 0)
    diagonal = iota((rows, rows), 0) // 8 == iota((rows, rows), 1) // 8
    gather = (iota((128, rows), 0) % 8 == iota((128, rows), 1) % 8).astype(BF)
    flipped = coupling[...].reshape(kinds * 64, 64).T
    upper = flipped.astype(BF)
    lower = (flipped - upper.astype(F32)).astype(BF)
    none = jnp.zeros_like(upper)
    for i, piece in enumerate((upper, upper, lower)):
        respond[i * 128 : i * 128 + 64, :] = jnp.concatenate([piece, none], axis=1)
        respond[i * 128 + 64 : i * 128 + 128, :] = jnp.concatenate([none, piece], axis=1)
    line = iota((n * pack, 64), 0)
    kind_of = []
    for parity in range(2):
        column = jnp.zeros((n * pack, 64), jnp.int32)
        for row in range(n * pack):
            owner = lax.rem(me - row // pack + n, n)
            kind = species[order[owner * own + (row % pack) * 2 + parity]]
            column = jnp.where(line == row, kind, column)
        kind_of.append(column)
    fan = (iota((8, 64), 1) % 8 == iota((8, 64), 0)).astype(F32)
    mine = iota((8, 64), 1) // 8 == iota((8, 64), 0)
    bare = [jnp.zeros((n * pack, 64), F32)] * 2
    for kind in range(kinds):
        flat = jnp.dot(base[kind], fan, precision=HIGH, preferred_element_type=F32)
        flat = jnp.sum(jnp.where(mine, flat, 0.0), axis=0, keepdims=True)
        for parity in range(2):
            bare[parity] = jnp.where(kind_of[parity] == kind, flat, bare[parity])
    member = iota((8, 128), 0) == (iota((8, 128), 1) % 64) // 8
    picks = [member & (iota((8, 128), 1) // 64 == parity) for parity in range(2)]

    total = part[block(me), :].astype(F32)
    for s in range(1, n):
        sends[s - 1].wait_recv()
        total = total + rs_in[s].astype(F32)
    p_all[0] = total.astype(BF)
    gram = lax.dot_general(
        total * weights, total, (((1,), (1,)), ((), ())), precision=HIGH, preferred_element_type=F32
    )
    gram = jnp.where(diagonal, gram, 0.0)
    occ8 = gram[0:8, :]
    for k in range(1, own):
        occ8 = occ8 + gram[k * 8 : k * 8 + 8, :]
    flat = jnp.dot(occ8, spread, precision=HIGH, preferred_element_type=F32)
    flat = jnp.sum(jnp.where(row_of, flat, 0.0), axis=0, keepdims=True)
    for r in range(pack):
        o_in[0, r : r + 1, :] = flat[:, r * 128 : r * 128 + 128]

    def occupancy_copy(q):
        return pltpu.make_async_remote_copy(
            src_ref=o_in.at[0],
            dst_ref=o_in.at[q],
            send_sem=oc_s.at[q],
            recv_sem=oc_r.at[q],
            device_id=place(q),
            device_id_type=MESH,
        )

    def tell(q, carry):
        occupancy_copy(q).start()
        return carry

    lax.fori_loop(1, peers, tell, 0)
    p_sends = []
    for s in range(1, n):
        copy = pltpu.make_async_remote_copy(
            src_ref=p_all.at[0],
            dst_ref=p_all.at[s],
            send_sem=ag_s.at[s],
            recv_sem=ag_r.at[s],
            device_id={"pw": lax.rem(me + s, n)},
            device_id_type=MESH,
        )
        copy.start()
        p_sends.append(copy)

    def hear(q, carry):
        occupancy_copy(q).wait_recv()
        return carry

    lax.fori_loop(1, peers, hear, 0)
    for d in range(n):
        summed = o_in[d * nb + lax.rem(mb + nb, nb)]
        for b in range(1, nb):
            summed = summed + o_in[d * nb + lax.rem(mb - b + nb, nb)]
        o_sum[d * pack : d * pack + pack, :] = summed
    summed = o_sum[...]
    upper = summed.astype(BF)
    lower = (summed - upper.astype(F32)).astype(BF)
    answer = jnp.dot(
        jnp.concatenate([upper, lower, upper], axis=1), respond[...], preferred_element_type=F32
    )
    matrix = []
    for parity in range(2):
        chosen = jnp.zeros((n * pack, 64), F32)
        for kind in range(kinds):
            at = (parity * kinds + kind) * 64
            chosen = jnp.where(kind_of[parity] == kind, answer[:, at : at + 64], chosen)
        matrix.append(bare[parity] + chosen)
    matrix = jnp.concatenate(matrix, axis=1)
    o_sum[...] = matrix

    for s in range(n):
        lines = []
        for k in range(own):
            at = s * pack + k // 2
            lines.append(
                jnp.where(picks[k % 2], jnp.broadcast_to(o_sum[at : at + 1, :], (8, 128)), 0.0)
            )
        lines = jnp.concatenate(lines, axis=0)
        upper = lines.astype(BF)
        lower = (lines - upper.astype(F32)).astype(BF)
        square = jnp.dot(
            jnp.concatenate([upper, lower], axis=0), gather, preferred_element_type=F32
        )
        upper = jnp.where(diagonal, square[0:rows, :], 0.0)
        lower = jnp.where(diagonal, square[rows : 2 * rows, :], 0.0)
        if s == 0:
            both = upper + lower
            for k in range(own):
                onsite[k] = both[k * 8 : k * 8 + 8, k * 8 : k * 8 + 8]
        if s:
            p_sends[s - 1].wait_recv()
        p = p_all[s]
        w = jnp.dot(
            jnp.concatenate([upper, lower], axis=0).astype(BF), p, preferred_element_type=F32
        )
        w = (w[0:rows, :] + w[rows : 2 * rows, :]).astype(BF)
        owner = lax.rem(me - s + n, n)
        ww[block(owner), :] = w
        second = pl.ds(pl.multiple_of(every + owner * rows, rows), rows)
        ww[second, 0:bands] = -w[:, bands : 2 * bands]
        ww[second, bands : 2 * bands] = w[:, 0:bands]
    result = jnp.dot(beta_t[...], ww[...], preferred_element_type=F32).astype(BF)
    applied[0] = result[:, 0:bands]
    applied[1] = result[:, bands : 2 * bands]
    for copy in sends + p_sends:
        copy.wait_send()

    def told(q, carry):
        occupancy_copy(q).wait_send()
        return carry

    lax.fori_loop(1, peers, told, 0)


def finish(applied_in, onsite_in, applied, onsite, sem):
    copies = [
        pltpu.make_async_copy(applied_in, applied, sem.at[0]),
        pltpu.make_async_copy(onsite_in, onsite, sem.at[1]),
    ]
    for copy in copies:
        copy.start()
    for copy in copies:
        copy.wait()


def solution(mesh):
    n, nb = mesh.shape["pw"], mesh.shape["band"]

    def local(wave, miller, reciprocal, fractional, species, order, widths, base, coupling, occ):
        _, npw, bands = wave.shape
        atoms = order.shape[0]
        own = atoms // n
        rows, every = own * 8, atoms * 8
        pack = own // 2
        kinds = widths.shape[0]
        vmem = pl.BlockSpec(memory_space=pltpu.VMEM)
        hbm = pl.BlockSpec(memory_space=pltpu.HBM)
        dma = pltpu.SemaphoreType.DMA
        results = (
            jax.ShapeDtypeStruct(wave.shape, BF),
            jax.ShapeDtypeStruct((own, 8, 8), F32),
        )
        first = pl.pallas_call(
            functools.partial(kernel, n, nb),
            out_shape=results,
            in_specs=[hbm] * 10,
            out_specs=(vmem, vmem),
            scratch_shapes=[
                pltpu.VMEM(miller.shape, jnp.int32),
                pltpu.SMEM(reciprocal.shape, F32),
                pltpu.SMEM(fractional.shape, F32),
                pltpu.SMEM(species.shape, jnp.int32),
                pltpu.SMEM(order.shape, jnp.int32),
                pltpu.SMEM(widths.shape, F32),
                pltpu.VMEM(base.shape, F32),
                pltpu.VMEM(coupling.shape, F32),
                pltpu.VMEM((1, bands), F32),
                pltpu.VMEM((2 * npw, 2 * bands), BF),
                pltpu.VMEM((atoms, npw), F32),
                pltpu.VMEM((atoms, npw), F32),
                pltpu.VMEM((atoms, npw), F32),
                pltpu.VMEM((kinds, 8, npw), F32),
                pltpu.VMEM((every, 2 * npw), BF),
                pltpu.VMEM((npw, 2 * every), BF),
                pltpu.VMEM((every, 2 * bands), BF),
                pltpu.VMEM((n, rows, 2 * bands), BF),
                pltpu.VMEM((n, rows, 2 * bands), BF),
                pltpu.VMEM((n * nb, pack, 128), F32),
                pltpu.VMEM((n * pack, 128), F32),
                pltpu.VMEM((384, kinds * 128), BF),
                pltpu.VMEM((2 * every, 2 * bands), BF),
                dma((12,)),
                dma((n,)),
                dma((n,)),
                dma((n,)),
                dma((n,)),
                dma((n * nb,)),
                dma((n * nb,)),
            ],
            compiler_params=pltpu.CompilerParams(
                collective_id=0, has_side_effects=True, vmem_limit_bytes=40 * 2**20
            ),
        )(
            *[
                pltpu.with_memory_space_constraint(value, pltpu.HBM)
                for value in (
                    wave,
                    miller,
                    reciprocal,
                    fractional,
                    species,
                    order,
                    widths,
                    base,
                    coupling,
                    occ.reshape(1, bands),
                )
            ]
        )
        anywhere = pl.BlockSpec(memory_space=pl.ANY)
        return pl.pallas_call(
            finish,
            out_shape=results,
            in_specs=[anywhere] * 2,
            out_specs=(hbm, hbm),
            scratch_shapes=[dma((2,))],
            compiler_params=pltpu.CompilerParams(vmem_limit_bytes=2**20),
        )(*first)

    placed = (P(None, "pw", "band"), P(None, "pw"), P(), P(), P(), P(), P(), P(), P(), P("band"))
    return jax.shard_map(
        local,
        mesh=mesh,
        in_specs=placed,
        out_specs=(P(None, "pw", "band"), P("pw", None, None)),
        check_vma=False,
    )
```

```python
import functools
import math

import jax
import jax.numpy as jnp
import numpy as np
from jax import lax
from jax.experimental import pallas as pl
from jax.experimental.pallas import tpu as pltpu
from jax.sharding import PartitionSpec as P

MESH = pl.DeviceIdType.MESH
HIGH = lax.Precision.HIGHEST
BF = jnp.bfloat16
F32 = jnp.float32


def even_fit(function, degree):
    nodes = 0.125 + 0.125 * np.cos(np.pi * (np.arange(64) + 0.5) / 64)
    fit = np.polynomial.Chebyshev.fit(nodes, function(np.sqrt(nodes)), degree, domain=[0.0, 0.25])
    return [float(c) for c in fit.convert(kind=np.polynomial.Polynomial, domain=[-1, 1]).coef]


COS = even_fit(lambda t: np.cos(2 * np.pi * t), 7)
SIN = even_fit(lambda t: np.sin(2 * np.pi * t) / t, 7)


def series(coefs, u):
    value = jnp.full_like(u, coefs[-1])
    for c in coefs[-2::-1]:
        value = value * u + c
    return value


def iota(shape, dim):
    return lax.broadcasted_iota(jnp.int32, shape, dim)


def kernel(
    n,
    nb,
    wave,
    miller_h,
    reciprocal_h,
    fractional_h,
    species_h,
    order_h,
    widths_h,
    base_h,
    coupling_h,
    occ_h,
    applied,
    onsite,
    miller,
    reciprocal,
    fractional,
    species,
    order,
    widths,
    base,
    coupling,
    occ,
    wv,
    xs,
    cs,
    sn,
    amp,
    beta,
    beta_t,
    part,
    rs_in,
    p_all,
    o_in,
    o_sum,
    respond,
    ww,
    load_sem,
    rs_s,
    rs_r,
    ag_s,
    ag_r,
    oc_s,
    oc_r,
    ready,
):
    me = lax.axis_index("pw")
    mb = lax.axis_index("band")
    npw = wave.shape[1]
    bands = wave.shape[2]
    atoms = order.shape[0]
    kinds = widths.shape[0]
    own = atoms // n
    pack = own // 2
    rows = own * 8
    every = atoms * 8
    peers = n * nb

    small = [
        (miller_h, miller),
        (reciprocal_h, reciprocal),
        (fractional_h, fractional),
        (species_h, species),
        (order_h, order),
        (widths_h, widths),
        (base_h, base),
        (coupling_h, coupling),
        (occ_h, occ),
        (wave.at[0], wv.at[pl.ds(0, npw), pl.ds(0, bands)]),
        (wave.at[1], wv.at[pl.ds(0, npw), pl.ds(bands, bands)]),
        (wave.at[1], wv.at[pl.ds(npw, npw), pl.ds(0, bands)]),
    ]
    loads = [
        pltpu.make_async_copy(source, to, load_sem.at[i]) for i, (source, to) in enumerate(small)
    ]
    for copy in loads:
        copy.start()
    barrier = pltpu.get_barrier_semaphore()

    def place(q):
        return {"pw": lax.rem(me + q // nb, n), "band": lax.rem(mb + lax.rem(q, nb), nb)}

    def each(step):
        if peers <= 64:
            for q in range(1, peers):
                step(q)
        else:
            lax.fori_loop(1, peers, lambda q, carry: (step(q), carry)[1], 0)

    for d in range(1, n):
        pl.semaphore_signal(
            barrier, inc=1, device_id={"pw": lax.rem(me + d, n)}, device_id_type=MESH
        )
    for b in range(1, nb):
        pl.semaphore_signal(
            barrier, inc=1, device_id={"band": lax.rem(mb + b, nb)}, device_id_type=MESH
        )
    for copy in loads[0:6]:
        copy.wait()

    m = [miller[c : c + 1, :].astype(F32) for c in range(3)]
    g = [
        (2.0 * math.pi)
        * (reciprocal[c, 0] * m[0] + reciprocal[c, 1] * m[1] + reciprocal[c, 2] * m[2])
        for c in range(3)
    ]
    g2 = g[0] * g[0] + g[1] * g[1] + g[2] * g[2]
    j = iota((8, npw), 0)
    is_s = j < 2
    wide = [jnp.broadcast_to(v, (8, npw)) for v in g]
    factor = jnp.where(
        (j == 2) | (j == 5), wide[0], jnp.where((j == 3) | (j == 6), wide[1], wide[2])
    )
    half = jnp.broadcast_to(-0.5 * g2, (8, npw))
    for s in range(widths.shape[0]):
        w = jnp.where(
            j == 0,
            widths[s, 0],
            jnp.where(j == 1, widths[s, 1], jnp.where(j < 5, widths[s, 2], widths[s, 3])),
        )
        amp[s] = jnp.where(is_s, 1.0, factor * w) * jnp.exp(half * (w * w))

    def position(k, carry):
        a = order[k]
        xs[pl.ds(k, 1), :] = (
            fractional[0, a] * m[0] + fractional[1, a] * m[1] + fractional[2, a] * m[2]
        )
        return carry

    lax.fori_loop(0, atoms, position, 0, unroll=8)
    x = xs[...]
    t = x - jnp.round(x)
    u = t * t
    cs[...] = series(COS, u)
    sn[...] = t * series(SIN, u)

    def projector(pair, carry):
        real, imag = [], []
        for e in range(2):
            k = pair * 2 + e
            c = jnp.broadcast_to(cs[pl.ds(k, 1), :], (8, npw))
            s = jnp.broadcast_to(sn[pl.ds(k, 1), :], (8, npw))
            a = amp[species[order[k]]]
            real.append(a * jnp.where(is_s, c, -s))
            imag.append(-a * jnp.where(is_s, s, c))
        at = pl.ds(pl.multiple_of(pair * 16, 16), 16)
        beta[at, 0:npw] = jnp.concatenate(real, axis=0).astype(BF)
        beta[at, npw : 2 * npw] = jnp.concatenate(imag, axis=0).astype(BF)
        return carry

    lax.fori_loop(0, atoms // 2, projector, 0, unroll=4)

    for copy in loads[6:]:
        copy.wait()
    wv[npw : 2 * npw, bands : 2 * bands] = -wv[0:npw, 0:bands]
    part[...] = jnp.dot(beta[...], wv[...], preferred_element_type=F32).astype(BF)
    pl.semaphore_wait(barrier, n - 1 + nb - 1)

    def block(index):
        return pl.ds(pl.multiple_of(index * rows, rows), rows)

    def scatter(s):
        to = lax.rem(me + s, n)
        return pltpu.make_async_remote_copy(
            src_ref=part.at[block(to)],
            dst_ref=rs_in.at[s],
            send_sem=rs_s.at[s],
            recv_sem=rs_r.at[s],
            device_id={"pw": to},
            device_id_type=MESH,
        )

    upper_half = me // (n // 2)
    far_first = [
        lax.rem(n - 2 - me + upper_half + (2 * upper_half - 1) * i + 2 * (n - 1), n - 1) + 1
        for i in range(n - 1)
    ]
    sends = [scatter(s) for s in range(1, n)]
    for s in far_first:
        scatter(s).start()
    for b in range(1, nb):
        pl.semaphore_signal(
            ready, inc=1, device_id={"band": lax.rem(mb + b, nb)}, device_id_type=MESH
        )

    beta_t[:, 0:every] = beta[:, 0:npw].T
    beta_t[:, every : 2 * every] = beta[:, npw : 2 * npw].T
    weights = occ[...] * (1.0 / (bands * nb))
    weights = jnp.concatenate([weights, weights], axis=1)
    spread = (
        (iota((rows, own * 64), 0) // 8 == iota((rows, own * 64), 1) // 64)
        & (iota((rows, own * 64), 0) % 8 == iota((rows, own * 64), 1) % 8)
    ).astype(F32)
    row_of = (iota((8, own * 64), 1) % 64) // 8 == iota((8, own * 64), 0)
    diagonal = iota((rows, rows), 0) // 8 == iota((rows, rows), 1) // 8
    gather = (iota((128, rows), 0) % 8 == iota((128, rows), 1) % 8).astype(BF)
    flipped = coupling[...].reshape(kinds * 64, 64).T
    upper = flipped.astype(BF)
    lower = (flipped - upper.astype(F32)).astype(BF)
    none = jnp.zeros_like(upper)
    for i, piece in enumerate((upper, upper, lower)):
        respond[i * 128 : i * 128 + 64, :] = jnp.concatenate([piece, none], axis=1)
        respond[i * 128 + 64 : i * 128 + 128, :] = jnp.concatenate([none, piece], axis=1)
    line = iota((n * pack, 64), 0)
    kind_of = []
    for parity in range(2):
        column = jnp.zeros((n * pack, 64), jnp.int32)
        for row in range(n * pack):
            owner = lax.rem(me - row // pack + n, n)
            kind = species[order[owner * own + (row % pack) * 2 + parity]]
            column = jnp.where(line == row, kind, column)
        kind_of.append(column)
    fan = (iota((8, 64), 1) % 8 == iota((8, 64), 0)).astype(F32)
    mine = iota((8, 64), 1) // 8 == iota((8, 64), 0)
    bare = [jnp.zeros((n * pack, 64), F32)] * 2
    for kind in range(kinds):
        flat = jnp.dot(base[kind], fan, precision=HIGH, preferred_element_type=F32)
        flat = jnp.sum(jnp.where(mine, flat, 0.0), axis=0, keepdims=True)
        for parity in range(2):
            bare[parity] = jnp.where(kind_of[parity] == kind, flat, bare[parity])
    member = iota((8, 128), 0) == (iota((8, 128), 1) % 64) // 8
    picks = [member & (iota((8, 128), 1) // 64 == parity) for parity in range(2)]

    pl.semaphore_wait(ready, nb - 1)
    total = part[block(me), :].astype(F32)
    for s in range(1, n):
        sends[s - 1].wait_recv()
        total = total + rs_in[s].astype(F32)
    p_all[0] = total.astype(BF)
    gram = lax.dot_general(
        total * weights, total, (((1,), (1,)), ((), ())), precision=HIGH, preferred_element_type=F32
    )
    gram = jnp.where(diagonal, gram, 0.0)
    occ8 = gram[0:8, :]
    for k in range(1, own):
        occ8 = occ8 + gram[k * 8 : k * 8 + 8, :]
    flat = jnp.dot(occ8, spread, precision=HIGH, preferred_element_type=F32)
    flat = jnp.sum(jnp.where(row_of, flat, 0.0), axis=0, keepdims=True)
    for r in range(pack):
        o_in[0, r : r + 1, :] = flat[:, r * 128 : r * 128 + 128]

    def occupancy_copy(q):
        return pltpu.make_async_remote_copy(
            src_ref=o_in.at[0],
            dst_ref=o_in.at[q],
            send_sem=oc_s.at[q],
            recv_sem=oc_r.at[q],
            device_id=place(q),
            device_id_type=MESH,
        )

    each(lambda q: occupancy_copy(q).start())
    p_sends = []
    for s in range(1, n):
        copy = pltpu.make_async_remote_copy(
            src_ref=p_all.at[0],
            dst_ref=p_all.at[s],
            send_sem=ag_s.at[s],
            recv_sem=ag_r.at[s],
            device_id={"pw": lax.rem(me + s, n)},
            device_id_type=MESH,
        )
        copy.start()
        p_sends.append(copy)

    each(lambda q: occupancy_copy(q).wait_recv())
    for d in range(n):
        summed = o_in[d * nb + lax.rem(mb + nb, nb)]
        for b in range(1, nb):
            summed = summed + o_in[d * nb + lax.rem(mb - b + nb, nb)]
        o_sum[d * pack : d * pack + pack, :] = summed
    summed = o_sum[...]
    upper = summed.astype(BF)
    lower = (summed - upper.astype(F32)).astype(BF)
    answer = jnp.dot(
        jnp.concatenate([upper, lower, upper], axis=1), respond[...], preferred_element_type=F32
    )
    matrix = []
    for parity in range(2):
        chosen = jnp.zeros((n * pack, 64), F32)
        for kind in range(kinds):
            at = (parity * kinds + kind) * 64
            chosen = jnp.where(kind_of[parity] == kind, answer[:, at : at + 64], chosen)
        matrix.append(bare[parity] + chosen)
    matrix = jnp.concatenate(matrix, axis=1)
    o_sum[...] = matrix

    for s in range(n):
        lines = []
        for k in range(own):
            at = s * pack + k // 2
            lines.append(
                jnp.where(picks[k % 2], jnp.broadcast_to(o_sum[at : at + 1, :], (8, 128)), 0.0)
            )
        lines = jnp.concatenate(lines, axis=0)
        upper = lines.astype(BF)
        lower = (lines - upper.astype(F32)).astype(BF)
        square = jnp.dot(
            jnp.concatenate([upper, lower], axis=0), gather, preferred_element_type=F32
        )
        upper = jnp.where(diagonal, square[0:rows, :], 0.0)
        lower = jnp.where(diagonal, square[rows : 2 * rows, :], 0.0)
        if s == 0:
            both = upper + lower
            for k in range(own):
                onsite[k] = both[k * 8 : k * 8 + 8, k * 8 : k * 8 + 8]
        if s:
            p_sends[s - 1].wait_recv()
        p = p_all[s]
        w = jnp.dot(
            jnp.concatenate([upper, lower], axis=0).astype(BF), p, preferred_element_type=F32
        )
        w = (w[0:rows, :] + w[rows : 2 * rows, :]).astype(BF)
        owner = lax.rem(me - s + n, n)
        ww[block(owner), :] = w
        second = pl.ds(pl.multiple_of(every + owner * rows, rows), rows)
        ww[second, 0:bands] = -w[:, bands : 2 * bands]
        ww[second, bands : 2 * bands] = w[:, 0:bands]
    result = jnp.dot(beta_t[...], ww[...], preferred_element_type=F32).astype(BF)
    applied[0] = result[:, 0:bands]
    applied[1] = result[:, bands : 2 * bands]
    for copy in sends + p_sends:
        copy.wait_send()
    each(lambda q: occupancy_copy(q).wait_send())


def finish(applied_in, onsite_in, applied, onsite, sem):
    copies = [
        pltpu.make_async_copy(applied_in, applied, sem.at[0]),
        pltpu.make_async_copy(onsite_in, onsite, sem.at[1]),
    ]
    for copy in copies:
        copy.start()
    for copy in copies:
        copy.wait()


def solution(mesh):
    n, nb = mesh.shape["pw"], mesh.shape["band"]

    def local(wave, miller, reciprocal, fractional, species, order, widths, base, coupling, occ):
        _, npw, bands = wave.shape
        atoms = order.shape[0]
        own = atoms // n
        rows, every = own * 8, atoms * 8
        pack = own // 2
        kinds = widths.shape[0]
        vmem = pl.BlockSpec(memory_space=pltpu.VMEM)
        hbm = pl.BlockSpec(memory_space=pltpu.HBM)
        dma = pltpu.SemaphoreType.DMA
        results = (
            jax.ShapeDtypeStruct(wave.shape, BF),
            jax.ShapeDtypeStruct((own, 8, 8), F32),
        )
        first = pl.pallas_call(
            functools.partial(kernel, n, nb),
            out_shape=results,
            in_specs=[hbm] * 10,
            out_specs=(vmem, vmem),
            scratch_shapes=[
                pltpu.VMEM(miller.shape, jnp.int32),
                pltpu.SMEM(reciprocal.shape, F32),
                pltpu.SMEM(fractional.shape, F32),
                pltpu.SMEM(species.shape, jnp.int32),
                pltpu.SMEM(order.shape, jnp.int32),
                pltpu.SMEM(widths.shape, F32),
                pltpu.VMEM(base.shape, F32),
                pltpu.VMEM(coupling.shape, F32),
                pltpu.VMEM((1, bands), F32),
                pltpu.VMEM((2 * npw, 2 * bands), BF),
                pltpu.VMEM((atoms, npw), F32),
                pltpu.VMEM((atoms, npw), F32),
                pltpu.VMEM((atoms, npw), F32),
                pltpu.VMEM((kinds, 8, npw), F32),
                pltpu.VMEM((every, 2 * npw), BF),
                pltpu.VMEM((npw, 2 * every), BF),
                pltpu.VMEM((every, 2 * bands), BF),
                pltpu.VMEM((n, rows, 2 * bands), BF),
                pltpu.VMEM((n, rows, 2 * bands), BF),
                pltpu.VMEM((n * nb, pack, 128), F32),
                pltpu.VMEM((n * pack, 128), F32),
                pltpu.VMEM((384, kinds * 128), BF),
                pltpu.VMEM((2 * every, 2 * bands), BF),
                dma((12,)),
                dma((n,)),
                dma((n,)),
                dma((n,)),
                dma((n,)),
                dma((n * nb,)),
                dma((n * nb,)),
                pltpu.SemaphoreType.REGULAR,
            ],
            compiler_params=pltpu.CompilerParams(
                collective_id=0, has_side_effects=True, vmem_limit_bytes=40 * 2**20
            ),
        )(
            *[
                pltpu.with_memory_space_constraint(value, pltpu.HBM)
                for value in (
                    wave,
                    miller,
                    reciprocal,
                    fractional,
                    species,
                    order,
                    widths,
                    base,
                    coupling,
                    occ.reshape(1, bands),
                )
            ]
        )
        anywhere = pl.BlockSpec(memory_space=pl.ANY)
        return pl.pallas_call(
            finish,
            out_shape=results,
            in_specs=[anywhere] * 2,
            out_specs=(hbm, hbm),
            scratch_shapes=[dma((2,))],
            compiler_params=pltpu.CompilerParams(vmem_limit_bytes=2**20),
        )(*first)

    placed = (P(None, "pw", "band"), P(None, "pw"), P(), P(), P(), P(), P(), P(), P(), P("band"))
    return jax.shard_map(
        local,
        mesh=mesh,
        in_specs=placed,
        out_specs=(P(None, "pw", "band"), P("pw", None, None)),
        check_vma=False,
    )
```
